32 devices in a mesh: tok: 8 (over z, x), exp: 4 (over y, core).
Axes of the slice: x: 2, y: 2, z: 4, core: 2. Of those that a mesh axis runs over, the one named last changes fastest.
Arguments:
- tokens: bfloat16 [16384, 7168], P('tok', 'exp'), may hold values from -6 to 6
- gate_weight: bfloat16 [7168, 256], P('exp'), may hold values from -0.0625 to 0.0625
- expert_ids: int32 [16384, 8], P('tok'), may hold values from 0 to 255, all different within a row
- expert_bias: float32 [256], P('exp'), may hold values from -0.002 to 0.002
Outputs:
- affinities: float32 [16384, 256], P('tok', 'exp')
- weights: float32 [16384, 8], P('tok')
- load: float32 [256], replicated
- new_bias: float32 [256], replicated
The draws below stay inside these ranges and needn't reach their ends.
All inputs are finite; a program needn't handle non-finite values.
Results may differ from the reference program's by a relative error of at most 0.0003.
Values may be sent and summed in bfloat16 or wider, within the bound.
A program may use at most 64 MiB of HBM per device.

```python
import jax
import jax.numpy as jnp
from jax import lax

D = 7168
E = 256
TOPK = 8
TOKENS = 16384


def block_scale(rng, extent, shards, low, high):
    def one(axis_at, blocks):
        draws = jax.random.uniform(jax.random.fold_in(jax.random.fold_in(rng, 6), axis_at), (blocks,), jnp.float32, low / len(shards), high / len(shards))
        return jnp.repeat(jnp.exp(draws), extent[axis_at] // blocks).reshape((-1,) + (1,) * (len(extent) - axis_at - 1))

    loudness = one(*shards[0])
    for cut in shards[1:]:
        loudness = loudness * one(*cut)
    return loudness


def picks_of(stream_key, rows, count, top, lift):
    ranking = jax.random.permutation(jax.random.fold_in(stream_key, 1), count)
    boost = ranking
    for power in range(3):
        boost = boost * boost // count
    boost = boost * lift // count
    tickets = jax.random.randint(jax.random.fold_in(stream_key, 2), (rows, count), 0, 4096) + boost
    holders = jax.random.permutation(jax.random.fold_in(stream_key, 3), rows)[jnp.arange(count) % rows]
    tickets = jnp.where(jnp.arange(rows)[:, None] == holders[None, :], 1 << 14, tickets)
    priority = tickets * count + jnp.arange(count)
    return lax.top_k(priority.astype(jnp.int32), top)[1].astype(jnp.int32)


def gaussian(own_key, shape, deviation, bound, shards=(), kind=jnp.bfloat16):
    loudness = block_scale(own_key, shape, shards, -0.22, 0.18) if shards else 1.0
    values = jax.random.normal(own_key, shape, jnp.float32) * deviation * loudness
    return jnp.minimum(jnp.maximum(values, -bound), bound).astype(kind)


def setup_inputs(seed: int = 0) -> dict:
    key_of = jax.random.split(jax.random.key(seed), 5)
    tokens = gaussian(key_of[0], (TOKENS, D), 1.0, 6.0, ((0, 8), (1, 4)))
    gate_weight = gaussian(key_of[1], (D, E), D ** -0.5, 0.0625, ((0, 4),))
    expert_ids = picks_of(key_of[2], TOKENS, E, TOPK, 512)
    expert_bias = jnp.clip(jax.random.uniform(key_of[3], (E,), jnp.float32, -0.002, 0.002) * block_scale(key_of[3], (E,), ((0, 4),), -0.4, 0.0), -0.002, 0.002)
    return {"tokens": tokens, "gate_weight": gate_weight, "expert_ids": expert_ids, "expert_bias": expert_bias}


def reference(tokens, gate_weight, expert_ids, expert_bias):
    logits = jnp.dot(tokens, gate_weight, preferred_element_type=jnp.float32)
    affinities = jax.nn.sigmoid(logits)
    chosen = jnp.take_along_axis(affinities, expert_ids, axis=1)
    weights = 2.5 * chosen / jnp.sum(chosen, axis=1, keepdims=True)
    numbers = jnp.arange(E, dtype=jnp.int32)
    load = jnp.sum((expert_ids[:, :, None] == numbers[None, None, :]).astype(jnp.float32), axis=(0, 1))
    target = jnp.float32(TOKENS * TOPK)
    new_bias = expert_bias + 0.001 * jnp.sign(target - jnp.float32(E) * load)
    return affinities, weights, load, new_bias
```

```python
import functools

import jax
import jax.numpy as jnp
from jax import lax
from jax.experimental import pallas as pl
from jax.experimental.pallas import tpu as pltpu
from jax.sharding import PartitionSpec as P

MESH = pl.DeviceIdType.MESH
F32 = jnp.float32
LINK = jnp.int16
TOP_CODE = 32760.0
TOKEN_BOUND, GATE_BOUND = 6.0, 0.0625


def kernel(ntok, widths, x_hbm, w_hbm, ids_hbm, bias_hbm,
           aff_hbm, wts_hbm, load_ref, newb_ref,
           xv, wv, wt, ids, bias_own, bias_all, part, rx1, keep, tx2, rx2, mine, lin, lrx,
           affv, wtsv, cnt,
           x_sem, w_sem, i_sem, b_sem, s1, r1, s2, r2, s4, r4, sc, rc, sb, rb, ao, wo):
    own = bias_own.shape[1]
    n = len(widths)
    starts = [sum(widths[:i]) for i in range(n)]
    t, e = lax.axis_index("tok"), lax.axis_index("exp")
    y, c = e // 2, e % 2
    mate = 2 * y + 1 - c
    peer = 2 * (1 - y) + c
    cross = 2 * (1 - y) + 1 - c
    experts = 4 * own

    def cols(i):
        return pl.ds(starts[i], widths[i])

    ids_in = pltpu.make_async_copy(ids_hbm, ids, i_sem)
    b_in = pltpu.make_async_copy(bias_hbm, bias_own, b_sem)
    w_in = pltpu.make_async_copy(w_hbm, wv, w_sem)
    x_in = [pltpu.make_async_copy(x_hbm.at[cols(i)], xv.at[cols(i)], x_sem.at[i]) for i in range(n)]
    ids_in.start()
    b_in.start()
    w_in.start()
    for copy in x_in:
        copy.start()

    barrier = pltpu.get_barrier_semaphore()
    for other in (mate, peer, cross):
        pl.semaphore_signal(barrier, inc=1, device_id=(t, other), device_id_type=MESH)
    for d in range(1, ntok):
        pl.semaphore_signal(barrier, inc=1, device_id=((t + d) % ntok, e), device_id_type=MESH)

    w_in.wait()
    wt[...] = wv[...].T
    ids_in.wait()
    numbers = lax.broadcasted_iota(jnp.int32, (experts, 1), 0)
    lanes = 128
    acc = jnp.zeros((experts, lanes), F32)
    for g in range(ids.shape[1] // lanes):
        for j in range(ids.shape[0]):
            acc = acc + jnp.where(ids[j:j + 1, g * lanes:(g + 1) * lanes] == numbers, F32(1), F32(0))
    counts = lax.dot_general(jnp.ones((8, lanes), jnp.bfloat16), acc.astype(jnp.bfloat16),
                             (((1,), (1,)), ((), ())), preferred_element_type=F32)
    cnt[0] = counts.astype(jnp.int32)
    b_in.wait()
    bias_all[0] = jnp.broadcast_to(bias_own[...], bias_all.shape[1:])

    pl.semaphore_wait(barrier, 3 + ntok - 1)

    cnt_out = [pltpu.make_async_remote_copy(
        src_ref=cnt.at[0], dst_ref=cnt.at[d], send_sem=sc.at[d], recv_sem=rc.at[d],
        device_id=((t + d) % ntok, e), device_id_type=MESH) for d in range(1, ntok)]
    bias_out = [pltpu.make_async_remote_copy(
        src_ref=bias_own, dst_ref=bias_all.at[k, pl.ds(0, 1)], send_sem=sb.at[k], recv_sem=rb.at[k],
        device_id=(t, other), device_id_type=MESH) for k, other in ((1, mate), (2, peer), (3, cross))]
    for copy in cnt_out + bias_out:
        copy.start()

    def first(i):
        return pltpu.make_async_remote_copy(
            src_ref=part.at[:, 1 - c, :, cols(i)], dst_ref=rx1.at[:, :, cols(i)],
            send_sem=s1.at[i], recv_sem=r1.at[i], device_id=(t, mate), device_id_type=MESH)

    def second(i):
        return pltpu.make_async_remote_copy(
            src_ref=tx2.at[:, cols(i)], dst_ref=rx2.at[:, cols(i)],
            send_sem=s2.at[i], recv_sem=r2.at[i], device_id=(t, peer), device_id_type=MESH)

    def fourth(i):
        return pltpu.make_async_remote_copy(
            src_ref=lin.at[:, cols(i)], dst_ref=lrx.at[:, cols(i)],
            send_sem=s4.at[i], recv_sem=r4.at[i], device_id=(t, mate), device_id_type=MESH)

    local = lax.broadcasted_iota(jnp.int32, (own, 1), 0)

    def pick(i, values, block):
        rows = []
        base = local + block * own
        for j in range(ids.shape[0]):
            hit = ids[j:j + 1, cols(i)] == base
            rows.append(jnp.sum(jnp.where(hit, values, F32(0)), axis=0, keepdims=True))
        return jnp.concatenate(rows, axis=0)

    def stage_a(i):
        x_in[i].wait()
        r = lax.dot_general(wt[...], xv[cols(i)], (((1,), (1,)), ((), ())), preferred_element_type=F32)
        part[:, :, :, cols(i)] = r.reshape(2, 2, own, widths[i])
        first(i).start()

    grain = float(int(30000 / (2 * xv.shape[1] * TOKEN_BOUND * GATE_BOUND)))

    def step_of(whole):
        return whole * F32(1.0 / (grain * TOP_CODE))

    def stage_b(i):
        first(i).wait_recv()
        give = part[1 - y, c, :, cols(i)] + rx1[1 - y, :, cols(i)]
        held = part[y, c, :, cols(i)] + rx1[y, :, cols(i)]
        keep[:, cols(i)] = held
        largest = jnp.max(jnp.maximum(jnp.abs(give), jnp.abs(held)), axis=0, keepdims=True)
        whole = jnp.floor(largest * grain) + 1.0
        inverse = F32(grain * TOP_CODE) / whole
        code = jnp.round(give * inverse)
        chosen = jnp.round(pick(i, held, e) * inverse)
        tail = jnp.concatenate([chosen, jnp.broadcast_to(whole, chosen.shape)], axis=0)
        tx2[0:own, cols(i)] = code.astype(jnp.int32).astype(LINK)
        tx2[own:, cols(i)] = tail.astype(jnp.int32).astype(LINK)
        second(i).start()
        lin[:, cols(i)] = pick(i, code, peer) * step_of(whole)
        mine[:, cols(i)] = chosen * step_of(whole)

    out = {}

    def stage_c(i):
        second(i).wait_recv()
        code = rx2[0:own, cols(i)].astype(jnp.int32).astype(F32)
        tail = rx2[own:, cols(i)].astype(jnp.int32).astype(F32)
        top = ids.shape[0]
        step = step_of(tail[top:top + 1])
        logits = keep[:, cols(i)] + code * step
        ours = mine[:, cols(i)] + pick(i, code, e) * step
        theirs = lin[:, cols(i)] + tail[0:top] * step
        lin[:, cols(i)] = ours + theirs
        fourth(i).start()
        affv[:, cols(i)] = 1.0 / (1.0 + jnp.exp(-logits))
        out[i] = pltpu.make_async_copy(affv.at[:, cols(i)], aff_hbm.at[:, cols(i)], ao.at[i])
        out[i].start()

    def stage_d(i):
        fourth(i).wait_recv()
        chosen = 1.0 / (1.0 + jnp.exp(-(lin[:, cols(i)] + lrx[:, cols(i)])))
        wtsv[:, cols(i)] = 2.5 * chosen / jnp.sum(chosen, axis=0, keepdims=True)

    for step in range(n + 3):
        if step < n:
            stage_a(step)
        if 0 <= step - 1 < n:
            stage_b(step - 1)
        if step == n:
            for copy in cnt_out + bias_out:
                copy.wait()
            total = cnt[0]
            for d in range(1, ntok):
                total = total + cnt[d]
            load = total[0:1].astype(F32)
            load_ref[...] = load
            target = F32(ntok * ids.shape[1] * ids.shape[0])
            gap = target - F32(experts) * load
            sign = jnp.where(gap > 0, F32(1), jnp.where(gap < 0, F32(-1), F32(0)))
            b0, b1, b2, b3 = (bias_all[k, 0:1] for k in range(4))
            even = jnp.where(c == 0, b0, b1), jnp.where(c == 0, b1, b0)
            odd = jnp.where(c == 0, b2, b3), jnp.where(c == 0, b3, b2)
            low = [jnp.where(y == 0, p, q) for p, q in zip(even, odd)]
            high = [jnp.where(y == 0, q, p) for p, q in zip(even, odd)]
            bias = jnp.concatenate(low + high, axis=1)
            newb_ref[...] = bias + 0.001 * sign
        if 0 <= step - 3 < n:
            stage_c(step - 3)
        if 0 <= step - 4 < n:
            stage_d(step - 4)
    stage_d(n - 1)
    w_out = pltpu.make_async_copy(wtsv, wts_hbm, wo)
    w_out.start()
    for i in range(n):
        first(i).wait_send()
        second(i).wait_send()
        fourth(i).wait_send()
        out[i].wait()
    w_out.wait()


def local(ntok, tokens, gate_weight, expert_ids, expert_bias):
    rows, depth = tokens.shape
    experts = gate_weight.shape[1]
    own = expert_bias.shape[0]
    top = expert_ids.shape[1]
    piece = 256
    widths = [piece] * (rows // piece)
    n = len(widths)
    dma = pltpu.SemaphoreType.DMA
    vm = pltpu.VMEM
    any_ = pl.BlockSpec(memory_space=pl.ANY)
    vmem = pl.BlockSpec(memory_space=pltpu.VMEM)
    aff, wts, load, newb = pl.pallas_call(
        functools.partial(kernel, ntok, widths),
        out_shape=(
            jax.ShapeDtypeStruct((own, rows), F32),
            jax.ShapeDtypeStruct((top, rows), F32),
            jax.ShapeDtypeStruct((1, experts), F32),
            jax.ShapeDtypeStruct((1, experts), F32),
        ),
        in_specs=[any_] * 4,
        out_specs=(any_, any_, vmem, vmem),
        scratch_shapes=[
            vm((rows, depth), tokens.dtype), vm((depth, experts), gate_weight.dtype),
            vm((experts, depth), gate_weight.dtype), vm((top, rows), jnp.int32),
            vm((1, own), F32), vm((4, 8, own), F32),
            vm((2, 2, own, rows), F32), vm((2, own, rows), F32), vm((own, rows), F32),
            vm((own + 2 * top, rows), LINK), vm((own + 2 * top, rows), LINK),
            vm((top, rows), F32), vm((top, rows), F32), vm((top, rows), F32),
            vm((own, rows), F32), vm((top, rows), F32), vm((ntok, 8, experts), jnp.int32),
            dma((n,)), dma, dma, dma, dma((n,)), dma((n,)), dma((n,)), dma((n,)),
            dma((n,)), dma((n,)), dma((ntok,)), dma((ntok,)), dma((4,)), dma((4,)), dma((n,)), dma,
        ],
        compiler_params=pltpu.CompilerParams(
            collective_id=0, has_side_effects=True, vmem_limit_bytes=60 * 1024 * 1024),
    )(tokens, gate_weight, expert_ids.T, expert_bias.reshape(1, own))
    return aff.T, wts.T, load.reshape(experts), newb.reshape(experts)


def solution(mesh):
    in_specs = (P("tok", "exp"), P("exp", None), P("tok", None), P("exp"))
    out_specs = (P("tok", "exp"), P("tok", None), P(), P())
    return jax.shard_map(functools.partial(local, mesh.shape["tok"]), mesh=mesh,
                         in_specs=in_specs, out_specs=out_specs, check_vma=False)
```

```python
import functools

import jax
import jax.numpy as jnp
from jax import lax
from jax.experimental import pallas as pl
from jax.experimental.pallas import tpu as pltpu
from jax.sharding import PartitionSpec as P

MESH = pl.DeviceIdType.MESH
F32 = jnp.float32
LINK = jnp.int16
TOP_CODE = 32760.0
TOKEN_BOUND, GATE_BOUND = 6.0, 0.0625


def kernel(ntok, widths, x_hbm, w_hbm, ids_hbm, bias_hbm,
           affv, wtsv, load_ref, newb_ref,
           xv, wv, wt, ids, bias_own, bias_all, part, rx1, keep, tx2, rx2, mine, lin, lrx,
           cnt_a, cnt,
           x_sem, w_sem, i_sem, b_sem, s1, r1, s2, r2, s4, r4, sa, ra, sc, rc, sb, rb):
    own = bias_own.shape[1]
    n = len(widths)
    starts = [sum(widths[:i]) for i in range(n)]
    t, e = lax.axis_index("tok"), lax.axis_index("exp")
    y, c = e // 2, e % 2
    mate = 2 * y + 1 - c
    peer = 2 * (1 - y) + c
    cross = 2 * (1 - y) + 1 - c
    experts = 4 * own

    def cols(i):
        return pl.ds(starts[i], widths[i])

    ids_in = pltpu.make_async_copy(ids_hbm, ids, i_sem)
    b_in = pltpu.make_async_copy(bias_hbm, bias_own, b_sem)
    w_in = pltpu.make_async_copy(w_hbm, wv, w_sem)
    x_in = [pltpu.make_async_copy(x_hbm.at[cols(i)], xv.at[cols(i)], x_sem.at[i]) for i in range(n)]
    w_in.start()
    ids_in.start()
    b_in.start()
    ahead = 2
    for copy in x_in[:ahead]:
        copy.start()

    barrier = pltpu.get_barrier_semaphore()
    for other in (mate, peer, cross):
        pl.semaphore_signal(barrier, inc=1, device_id=(t, other), device_id_type=MESH)
    for d in range(1, ntok):
        pl.semaphore_signal(barrier, inc=1, device_id=((t + d) % ntok, e), device_id_type=MESH)

    ids_in.wait()
    lanes = 128
    share = ids.shape[1] // 4
    numbers = lax.broadcasted_iota(jnp.int32, (experts, lanes), 0).astype(F32).astype(jnp.bfloat16)
    one, zero = jnp.bfloat16(1), jnp.bfloat16(0)
    acc = jnp.zeros((experts, lanes), jnp.bfloat16)
    for g in range(share // lanes):
        at = pl.multiple_of(e * share + g * lanes, lanes)
        found = ids[:, pl.ds(at, lanes)].astype(F32).astype(jnp.bfloat16)
        for j in range(ids.shape[0]):
            acc = acc + jnp.where(found[j:j + 1] == numbers, one, zero)
    counts = lax.dot_general(jnp.ones((8, lanes), jnp.bfloat16), acc,
                             (((1,), (1,)), ((), ())), preferred_element_type=F32)
    cnt_a[0] = counts.astype(jnp.int32)
    b_in.wait()
    bias_all[0] = jnp.broadcast_to(bias_own[...], bias_all.shape[1:])
    w_in.wait()
    for copy in x_in[ahead:2 * ahead]:
        copy.start()
    wt[...] = wv[...].T

    pl.semaphore_wait(barrier, 3 + ntok - 1)

    group = ((1, mate), (2, peer), (3, cross))
    share_out = [pltpu.make_async_remote_copy(
        src_ref=cnt_a.at[0], dst_ref=cnt_a.at[k], send_sem=sa.at[k], recv_sem=ra.at[k],
        device_id=(t, other), device_id_type=MESH) for k, other in group]
    bias_out = [pltpu.make_async_remote_copy(
        src_ref=bias_own, dst_ref=bias_all.at[k, pl.ds(0, 1)], send_sem=sb.at[k], recv_sem=rb.at[k],
        device_id=(t, other), device_id_type=MESH) for k, other in group]
    cnt_out = [pltpu.make_async_remote_copy(
        src_ref=cnt.at[0], dst_ref=cnt.at[d], send_sem=sc.at[d], recv_sem=rc.at[d],
        device_id=((t + d) % ntok, e), device_id_type=MESH) for d in range(1, ntok)]
    for copy in share_out + bias_out:
        copy.start()

    def first(i):
        return pltpu.make_async_remote_copy(
            src_ref=part.at[:, 1 - c, :, cols(i)], dst_ref=rx1.at[:, :, cols(i)],
            send_sem=s1.at[i], recv_sem=r1.at[i], device_id=(t, mate), device_id_type=MESH)

    def second(i):
        return pltpu.make_async_remote_copy(
            src_ref=tx2.at[:, cols(i)], dst_ref=rx2.at[:, cols(i)],
            send_sem=s2.at[i], recv_sem=r2.at[i], device_id=(t, peer), device_id_type=MESH)

    def fourth(i):
        return pltpu.make_async_remote_copy(
            src_ref=lin.at[:, cols(i)], dst_ref=lrx.at[:, cols(i)],
            send_sem=s4.at[i], recv_sem=r4.at[i], device_id=(t, mate), device_id_type=MESH)

    local = lax.broadcasted_iota(jnp.int32, (own, 1), 0)

    def pick(i, values, block):
        rows = []
        base = local + block * own
        for j in range(ids.shape[0]):
            hit = ids[j:j + 1, cols(i)] == base
            rows.append(jnp.sum(jnp.where(hit, values, F32(0)), axis=0, keepdims=True))
        return jnp.concatenate(rows, axis=0)

    def stage_a(i):
        x_in[i].wait()
        if i + 2 * ahead < n:
            x_in[i + 2 * ahead].start()
        r = lax.dot_general(wt[...], xv[cols(i)], (((1,), (1,)), ((), ())), preferred_element_type=F32)
        part[:, :, :, cols(i)] = r.reshape(2, 2, own, widths[i])
        first(i).start()

    grain = float(int(30000 / (2 * xv.shape[1] * TOKEN_BOUND * GATE_BOUND)))

    def step_of(whole):
        return whole * F32(1.0 / (grain * TOP_CODE))

    def stage_b(i):
        first(i).wait_recv()
        give = part[1 - y, c, :, cols(i)] + rx1[1 - y, :, cols(i)]
        held = part[y, c, :, cols(i)] + rx1[y, :, cols(i)]
        keep[:, cols(i)] = held
        largest = jnp.max(jnp.maximum(jnp.abs(give), jnp.abs(held)), axis=0, keepdims=True)
        whole = jnp.floor(largest * grain) + 1.0
        inverse = F32(grain * TOP_CODE) / whole
        code = jnp.round(give * inverse)
        chosen = jnp.round(pick(i, held, e) * inverse)
        tail = jnp.concatenate([chosen, jnp.broadcast_to(whole, chosen.shape)], axis=0)
        tx2[0:own, cols(i)] = code.astype(jnp.int32).astype(LINK)
        tx2[own:, cols(i)] = tail.astype(jnp.int32).astype(LINK)
        second(i).start()
        lin[:, cols(i)] = pick(i, code, peer) * step_of(whole)
        mine[:, cols(i)] = chosen * step_of(whole)

    def stage_c(i):
        second(i).wait_recv()
        code = rx2[0:own, cols(i)].astype(jnp.int32).astype(F32)
        tail = rx2[own:, cols(i)].astype(jnp.int32).astype(F32)
        top = ids.shape[0]
        step = step_of(tail[top:top + 1])
        logits = keep[:, cols(i)] + code * step
        ours = mine[:, cols(i)] + pick(i, code, e) * step
        theirs = lin[:, cols(i)] + tail[0:top] * step
        lin[:, cols(i)] = ours + theirs
        fourth(i).start()
        affv[:, cols(i)] = 1.0 / (1.0 + jnp.exp(-logits))

    def stage_d(i):
        fourth(i).wait_recv()
        chosen = 1.0 / (1.0 + jnp.exp(-(lin[:, cols(i)] + lrx[:, cols(i)])))
        wtsv[:, cols(i)] = 2.5 * chosen / jnp.sum(chosen, axis=0, keepdims=True)

    def merge_counts():
        for copy in share_out:
            copy.wait()
        cnt[0] = (cnt_a[0] + cnt_a[1]) + (cnt_a[2] + cnt_a[3])
        for copy in cnt_out:
            copy.start()

    def finish_counts():
        for copy in cnt_out + bias_out:
            copy.wait()
        total = cnt[0]
        for d in range(1, ntok):
            total = total + cnt[d]
        load = total[0:1].astype(F32)
        load_ref[...] = load
        target = F32(ntok * ids.shape[1] * ids.shape[0])
        gap = target - F32(experts) * load
        sign = jnp.where(gap > 0, F32(1), jnp.where(gap < 0, F32(-1), F32(0)))
        b0, b1, b2, b3 = (bias_all[k, 0:1] for k in range(4))
        near = jnp.where(c == 0, b0, b1), jnp.where(c == 0, b1, b0)
        far = jnp.where(c == 0, b2, b3), jnp.where(c == 0, b3, b2)
        low = [jnp.where(y == 0, p, q) for p, q in zip(near, far)]
        high = [jnp.where(y == 0, q, p) for p, q in zip(near, far)]
        bias = jnp.concatenate(low + high, axis=1)
        newb_ref[...] = bias + 0.001 * sign

    lag_b, lag_c, lag_d = 2, 7, 8
    for step in range(n + lag_d):
        if step < n:
            stage_a(step)
        if 0 <= step - lag_b < n:
            stage_b(step - lag_b)
        if step == n // 2:
            merge_counts()
        if step == n + lag_b:
            finish_counts()
        if 0 <= step - lag_c < n:
            stage_c(step - lag_c)
        if 0 <= step - lag_d < n:
            stage_d(step - lag_d)
    for i in range(n):
        first(i).wait_send()
        second(i).wait_send()
        fourth(i).wait_send()


def local(ntok, tokens, gate_weight, expert_ids, expert_bias):
    rows, depth = tokens.shape
    experts = gate_weight.shape[1]
    own = expert_bias.shape[0]
    top = expert_ids.shape[1]
    piece = 256
    widths = [piece] * (rows // piece)
    n = len(widths)
    dma = pltpu.SemaphoreType.DMA
    vm = pltpu.VMEM
    any_ = pl.BlockSpec(memory_space=pl.ANY)
    vmem = pl.BlockSpec(memory_space=pltpu.VMEM)
    shapes = ((own, rows), (top, rows), (1, experts), (1, experts))
    results = pl.pallas_call(
        functools.partial(kernel, ntok, widths),
        out_shape=tuple(pltpu.VMEM(shape, F32) for shape in shapes),
        in_specs=[any_] * 4,
        out_specs=(vmem,) * 4,
        scratch_shapes=[
            vm((rows, depth), tokens.dtype), vm((depth, experts), gate_weight.dtype),
            vm((experts, depth), gate_weight.dtype), vm((top, rows), jnp.int32),
            vm((1, own), F32), vm((4, 8, own), F32),
            vm((2, 2, own, rows), F32), vm((2, own, rows), F32), vm((own, rows), F32),
            vm((own + 2 * top, rows), LINK), vm((own + 2 * top, rows), LINK),
            vm((top, rows), F32), vm((top, rows), F32), vm((top, rows), F32),
            vm((4, 8, experts), jnp.int32), vm((ntok, 8, experts), jnp.int32),
            dma((n,)), dma, dma, dma, dma((n,)), dma((n,)), dma((n,)), dma((n,)),
            dma((n,)), dma((n,)), dma((4,)), dma((4,)), dma((ntok,)), dma((ntok,)), dma((4,)), dma((4,)),
        ],
        compiler_params=pltpu.CompilerParams(
            collective_id=0, has_side_effects=True, vmem_limit_bytes=60 * 1024 * 1024),
    )(tokens, gate_weight, expert_ids.T, expert_bias.reshape(1, own))
    aff, wts, load, newb = results
    return aff.T, wts.T, load.reshape(experts), newb.reshape(experts)


def solution(mesh):
    in_specs = (P("tok", "exp"), P("exp", None), P("tok", None), P("exp"))
    out_specs = (P("tok", "exp"), P("tok", None), P(), P())
    return jax.shard_map(functools.partial(local, mesh.shape["tok"]), mesh=mesh,
                         in_specs=in_specs, out_specs=out_specs, check_vma=False)
```

```python
import functools

import jax
import jax.numpy as jnp
from jax import lax
from jax.experimental import pallas as pl
from jax.experimental.pallas import tpu as pltpu
from jax.sharding import PartitionSpec as P

MESH = pl.DeviceIdType.MESH
F32 = jnp.float32
LINK = jnp.int16
TOP_CODE = 32760.0
TOKEN_BOUND, GATE_BOUND = 6.0, 0.0625


def kernel(ntok, widths, x_hbm, w_hbm, ids_hbm, bias_hbm,
           affv, wtsv, load_ref, newb_ref,
           xv, wv, wt, ids, bias_own, bias_all, part, rx1, keep, tx2, rx2, mine, lin, lrx,
           cnt_a, cnt,
           x_sem, w_sem, i_sem, b_sem, s1, r1, s2, r2, s4, r4, sa, ra, sc, rc, sb, rb):
    own = bias_own.shape[1]
    n = len(widths)
    starts = [sum(widths[:i]) for i in range(n)]
    t, e = lax.axis_index("tok"), lax.axis_index("exp")
    y, c = e // 2, e % 2
    mate = 2 * y + 1 - c
    peer = 2 * (1 - y) + c
    cross = 2 * (1 - y) + 1 - c
    experts = 4 * own

    def cols(i):
        return pl.ds(starts[i], widths[i])

    ids_in = pltpu.make_async_copy(ids_hbm, ids, i_sem)
    b_in = pltpu.make_async_copy(bias_hbm, bias_own, b_sem)
    w_in = pltpu.make_async_copy(w_hbm, wv, w_sem)
    x_in = [pltpu.make_async_copy(x_hbm.at[cols(i)], xv.at[cols(i)], x_sem.at[i]) for i in range(n)]
    w_in.start()
    ids_in.start()
    b_in.start()
    ahead = 2
    for copy in x_in[:ahead]:
        copy.start()

    barrier = pltpu.get_barrier_semaphore()
    for other in (mate, peer, cross):
        pl.semaphore_signal(barrier, inc=1, device_id=(t, other), device_id_type=MESH)
    for d in range(1, ntok):
        pl.semaphore_signal(barrier, inc=1, device_id=((t + d) % ntok, e), device_id_type=MESH)

    ids_in.wait()
    lanes = 128
    share = ids.shape[1] // 4
    numbers = lax.broadcasted_iota(jnp.int32, (experts, lanes), 0).astype(F32).astype(jnp.bfloat16)
    one, zero = jnp.bfloat16(1), jnp.bfloat16(0)
    acc = jnp.zeros((experts, lanes), jnp.bfloat16)
    for g in range(share // lanes):
        at = pl.multiple_of(e * share + g * lanes, lanes)
        found = ids[:, pl.ds(at, lanes)].astype(F32).astype(jnp.bfloat16)
        for j in range(ids.shape[0]):
            acc = acc + jnp.where(found[j:j + 1] == numbers, one, zero)
    counts = lax.dot_general(jnp.ones((8, lanes), jnp.bfloat16), acc,
                             (((1,), (1,)), ((), ())), preferred_element_type=F32)
    cnt_a[0] = counts.astype(jnp.int32)
    b_in.wait()
    bias_all[0] = jnp.broadcast_to(bias_own[...], bias_all.shape[1:])
    w_in.wait()
    for copy in x_in[ahead:2 * ahead]:
        copy.start()
    wt[...] = wv[...].T

    pl.semaphore_wait(barrier, 3 + ntok - 1)

    group = ((1, mate), (2, peer), (3, cross))
    share_out = [pltpu.make_async_remote_copy(
        src_ref=cnt_a.at[0], dst_ref=cnt_a.at[k], send_sem=sa.at[k], recv_sem=ra.at[k],
        device_id=(t, other), device_id_type=MESH) for k, other in group]
    bias_out = [pltpu.make_async_remote_copy(
        src_ref=bias_own, dst_ref=bias_all.at[k, pl.ds(0, 1)], send_sem=sb.at[k], recv_sem=rb.at[k],
        device_id=(t, other), device_id_type=MESH) for k, other in group]
    cnt_out = [pltpu.make_async_remote_copy(
        src_ref=cnt.at[0], dst_ref=cnt.at[d], send_sem=sc.at[d], recv_sem=rc.at[d],
        device_id=((t + d) % ntok, e), device_id_type=MESH) for d in range(1, ntok)]
    for copy in share_out + bias_out:
        copy.start()

    def first(i):
        return pltpu.make_async_remote_copy(
            src_ref=part.at[:, 1 - c, :, cols(i)], dst_ref=rx1.at[:, :, cols(i)],
            send_sem=s1.at[i], recv_sem=r1.at[i], device_id=(t, mate), device_id_type=MESH)

    def second(i):
        return pltpu.make_async_remote_copy(
            src_ref=tx2.at[:, cols(i)], dst_ref=rx2.at[:, cols(i)],
            send_sem=s2.at[i], recv_sem=r2.at[i], device_id=(t, peer), device_id_type=MESH)

    def fourth(i):
        return pltpu.make_async_remote_copy(
            src_ref=lin.at[:, cols(i)], dst_ref=lrx.at[:, cols(i)],
            send_sem=s4.at[i], recv_sem=r4.at[i], device_id=(t, mate), device_id_type=MESH)

    local = lax.broadcasted_iota(jnp.int32, (own, 1), 0)

    def pick(i, values, block):
        rows = []
        base = local + block * own
        for j in range(ids.shape[0]):
            hit = ids[j:j + 1, cols(i)] == base
            rows.append(jnp.sum(jnp.where(hit, values, F32(0)), axis=0, keepdims=True))
        return jnp.concatenate(rows, axis=0)

    def stage_a(i):
        x_in[i].wait()
        if i + 2 * ahead < n:
            x_in[i + 2 * ahead].start()
        r = lax.dot_general(wt[...], xv[cols(i)], (((1,), (1,)), ((), ())), preferred_element_type=F32)
        part[:, :, :, cols(i)] = r.reshape(2, 2, own, widths[i])
        first(i).start()

    grain = float(int(30000 / (2 * xv.shape[1] * TOKEN_BOUND * GATE_BOUND)))

    def step_of(whole):
        return whole * F32(1.0 / (grain * TOP_CODE))

    def stage_b(i):
        first(i).wait_recv()
        give = part[1 - y, c, :, cols(i)] + rx1[1 - y, :, cols(i)]
        held = part[y, c, :, cols(i)] + rx1[y, :, cols(i)]
        keep[:, cols(i)] = held
        largest = jnp.max(jnp.maximum(jnp.abs(give), jnp.abs(held)), axis=0, keepdims=True)
        whole = jnp.floor(largest * grain) + 1.0
        inverse = F32(grain * TOP_CODE) / whole
        code = jnp.round(give * inverse)
        chosen = jnp.round(pick(i, held, e) * inverse)
        tail = jnp.concatenate([chosen, jnp.broadcast_to(whole, chosen.shape)], axis=0)
        tx2[0:own, cols(i)] = code.astype(jnp.int32).astype(LINK)
        tx2[own:, cols(i)] = tail.astype(jnp.int32).astype(LINK)
        second(i).start()
        lin[:, cols(i)] = pick(i, code, peer) * step_of(whole)
        mine[:, cols(i)] = chosen * step_of(whole)

    def stage_c(i):
        second(i).wait_recv()
        code = rx2[0:own, cols(i)].astype(jnp.int32).astype(F32)
        tail = rx2[own:, cols(i)].astype(jnp.int32).astype(F32)
        top = ids.shape[0]
        step = step_of(tail[top:top + 1])
        logits = keep[:, cols(i)] + code * step
        ours = mine[:, cols(i)] + pick(i, code, e) * step
        theirs = lin[:, cols(i)] + tail[0:top] * step
        lin[:, cols(i)] = ours + theirs
        fourth(i).start()
        affv[:, cols(i)] = 1.0 / (1.0 + jnp.exp(-logits))

    def stage_d(i):
        fourth(i).wait_recv()
        chosen = 1.0 / (1.0 + jnp.exp(-(lin[:, cols(i)] + lrx[:, cols(i)])))
        wtsv[:, cols(i)] = 2.5 * chosen / jnp.sum(chosen, axis=0, keepdims=True)

    def merge_counts():
        for copy in share_out:
            copy.wait()
        cnt[0] = (cnt_a[0] + cnt_a[1]) + (cnt_a[2] + cnt_a[3])
        for copy in cnt_out:
            copy.start()

    def finish_counts():
        for copy in cnt_out + bias_out:
            copy.wait()
        total = cnt[0]
        for d in range(1, ntok):
            total = total + cnt[d]
        load = total[0:1].astype(F32)
        load_ref[...] = load
        target = F32(ntok * ids.shape[1] * ids.shape[0])
        gap = target - F32(experts) * load
        sign = jnp.where(gap > 0, F32(1), jnp.where(gap < 0, F32(-1), F32(0)))
        b0, b1, b2, b3 = (bias_all[k, 0:1] for k in range(4))
        near = jnp.where(c == 0, b0, b1), jnp.where(c == 0, b1, b0)
        far = jnp.where(c == 0, b2, b3), jnp.where(c == 0, b3, b2)
        low = [jnp.where(y == 0, p, q) for p, q in zip(near, far)]
        high = [jnp.where(y == 0, q, p) for p, q in zip(near, far)]
        bias = jnp.concatenate(low + high, axis=1)
        newb_ref[...] = bias + 0.001 * sign

    lag_b, lag_c, lag_d = 2, 7, 8
    for step in range(n + lag_d):
        if step < n:
            stage_a(step)
        if 0 <= step - lag_b < n:
            stage_b(step - lag_b)
        if step == n // 2:
            merge_counts()
        if step == n + lag_b:
            finish_counts()
        if 0 <= step - lag_c < n:
            stage_c(step - lag_c)
        if 0 <= step - lag_d < n:
            stage_d(step - lag_d)
    for i in range(n):
        first(i).wait_send()
        second(i).wait_send()
        fourth(i).wait_send()


def place(aff, wts, load, newb, aff_hbm, wts_hbm, load_hbm, newb_hbm, sem):
    copies = [pltpu.make_async_copy(a, b, sem.at[k]) for k, (a, b) in enumerate(
        ((aff, aff_hbm), (wts, wts_hbm), (load, load_hbm), (newb, newb_hbm)))]
    for copy in copies:
        copy.start()
    for copy in copies:
        copy.wait()


def local(ntok, tokens, gate_weight, expert_ids, expert_bias):
    rows, depth = tokens.shape
    experts = gate_weight.shape[1]
    own = expert_bias.shape[0]
    top = expert_ids.shape[1]
    piece = 256
    widths = [piece // 2] * 2 + [piece] * (rows // piece - 1)
    n = len(widths)
    dma = pltpu.SemaphoreType.DMA
    vm = pltpu.VMEM
    any_ = pl.BlockSpec(memory_space=pl.ANY)
    vmem = pl.BlockSpec(memory_space=pltpu.VMEM)
    shapes = ((own, rows), (top, rows), (1, experts), (1, experts))
    results = pl.pallas_call(
        functools.partial(kernel, ntok, widths),
        out_shape=tuple(pltpu.VMEM(shape, F32) for shape in shapes),
        in_specs=[any_] * 4,
        out_specs=(vmem,) * 4,
        scratch_shapes=[
            vm((rows, depth), tokens.dtype), vm((depth, experts), gate_weight.dtype),
            vm((experts, depth), gate_weight.dtype), vm((top, rows), jnp.int32),
            vm((1, own), F32), vm((4, 8, own), F32),
            vm((2, 2, own, rows), F32), vm((2, own, rows), F32), vm((own, rows), F32),
            vm((own + 2 * top, rows), LINK), vm((own + 2 * top, rows), LINK),
            vm((top, rows), F32), vm((top, rows), F32), vm((top, rows), F32),
            vm((4, 8, experts), jnp.int32), vm((ntok, 8, experts), jnp.int32),
            dma((n,)), dma, dma, dma, dma((n,)), dma((n,)), dma((n,)), dma((n,)),
            dma((n,)), dma((n,)), dma((4,)), dma((4,)), dma((ntok,)), dma((ntok,)), dma((4,)), dma((4,)),
        ],
        compiler_params=pltpu.CompilerParams(
            collective_id=0, has_side_effects=True, vmem_limit_bytes=60 * 1024 * 1024),
    )(tokens, gate_weight, expert_ids.T, expert_bias.reshape(1, own))
    aff, wts, load, newb = pl.pallas_call(
        place,
        out_shape=tuple(jax.ShapeDtypeStruct(shape, F32) for shape in shapes),
        in_specs=[vmem] * 4,
        out_specs=(pl.BlockSpec(memory_space=pltpu.HBM),) * 4,
        scratch_shapes=[dma((4,))],
    )(*(pltpu.with_memory_space_constraint(r, pltpu.VMEM) for r in results))
    return aff.T, wts.T, load.reshape(experts), newb.reshape(experts)


def solution(mesh):
    in_specs = (P("tok", "exp"), P("exp", None), P("tok", None), P("exp"))
    out_specs = (P("tok", "exp"), P("tok", None), P(), P())
    return jax.shard_map(functools.partial(local, mesh.shape["tok"]), mesh=mesh,
                         in_specs=in_specs, out_specs=out_specs, check_vma=False)
```

```python
import functools

import jax
import jax.numpy as jnp
from jax import lax
from jax.experimental import pallas as pl
from jax.experimental.pallas import tpu as pltpu
from jax.sharding import PartitionSpec as P

MESH = pl.DeviceIdType.MESH
F32 = jnp.float32
LINK = jnp.int16
TOP_CODE = 32760.0
TOKEN_BOUND, GATE_BOUND = 6.0, 0.0625


def kernel(ntok, widths, x_hbm, w_hbm, ids_hbm, bias_hbm,
           affv, wtsv, load_ref, newb_ref,
           xv, wv, wt, ids, bias_own, bias_all, part, rx1, keep, tx2, rx2, mine, lin, lrx,
           cnt_a, cnt,
           x_sem, w_sem, i_sem, b_sem, s1, r1, s2, r2, s4, r4, sa, ra, sc, rc, sb, rb):
    own = bias_own.shape[1]
    n = len(widths)
    starts = [sum(widths[:i]) for i in range(n)]
    t, e = lax.axis_index("tok"), lax.axis_index("exp")
    y, c = e // 2, e % 2
    mate = 2 * y + 1 - c
    peer = 2 * (1 - y) + c
    cross = 2 * (1 - y) + 1 - c
    experts = 4 * own

    def cols(i):
        return pl.ds(starts[i], widths[i])

    ids_in = pltpu.make_async_copy(ids_hbm, ids, i_sem)
    b_in = pltpu.make_async_copy(bias_hbm, bias_own, b_sem)
    w_in = pltpu.make_async_copy(w_hbm, wv, w_sem)
    x_in = [pltpu.make_async_copy(x_hbm.at[cols(i)], xv.at[cols(i)], x_sem.at[i]) for i in range(n)]
    w_in.start()
    ids_in.start()
    b_in.start()
    ahead = 3
    for copy in x_in[:ahead]:
        copy.start()

    barrier = pltpu.get_barrier_semaphore()
    for other in (mate, peer, cross):
        pl.semaphore_signal(barrier, inc=1, device_id=(t, other), device_id_type=MESH)
    for d in range(1, ntok):
        pl.semaphore_signal(barrier, inc=1, device_id=((t + d) % ntok, e), device_id_type=MESH)

    ids_in.wait()
    lanes = 128
    share = ids.shape[1] // 4
    numbers = lax.broadcasted_iota(jnp.int32, (experts, lanes), 0).astype(F32).astype(jnp.bfloat16)
    one, zero = jnp.bfloat16(1), jnp.bfloat16(0)
    acc = jnp.zeros((experts, lanes), jnp.bfloat16)
    for g in range(share // lanes):
        at = pl.multiple_of(e * share + g * lanes, lanes)
        found = ids[:, pl.ds(at, lanes)].astype(F32).astype(jnp.bfloat16)
        for j in range(ids.shape[0]):
            acc = acc + jnp.where(found[j:j + 1] == numbers, one, zero)
    counts = lax.dot_general(jnp.ones((8, lanes), jnp.bfloat16), acc,
                             (((1,), (1,)), ((), ())), preferred_element_type=F32)
    cnt_a[0] = counts.astype(jnp.int32)
    b_in.wait()
    bias_all[0] = jnp.broadcast_to(bias_own[...], bias_all.shape[1:])
    w_in.wait()
    for copy in x_in[ahead:2 * ahead]:
        copy.start()
    wt[...] = wv[...].T

    pl.semaphore_wait(barrier, 3 + ntok - 1)

    group = ((1, mate), (2, peer), (3, cross))
    share_out = [pltpu.make_async_remote_copy(
        src_ref=cnt_a.at[0], dst_ref=cnt_a.at[k], send_sem=sa.at[k], recv_sem=ra.at[k],
        device_id=(t, other), device_id_type=MESH) for k, other in group]
    bias_out = [pltpu.make_async_remote_copy(
        src_ref=bias_own, dst_ref=bias_all.at[k, pl.ds(0, 1)], send_sem=sb.at[k], recv_sem=rb.at[k],
        device_id=(t, other), device_id_type=MESH) for k, other in group]
    cnt_out = [pltpu.make_async_remote_copy(
        src_ref=cnt.at[0], dst_ref=cnt.at[d], send_sem=sc.at[d], recv_sem=rc.at[d],
        device_id=((t + d) % ntok, e), device_id_type=MESH) for d in range(1, ntok)]
    for copy in share_out + bias_out:
        copy.start()

    def first(i):
        return pltpu.make_async_remote_copy(
            src_ref=part.at[:, 1 - c, :, cols(i)], dst_ref=rx1.at[:, :, cols(i)],
            send_sem=s1.at[i], recv_sem=r1.at[i], device_id=(t, mate), device_id_type=MESH)

    def second(i):
        return pltpu.make_async_remote_copy(
            src_ref=tx2.at[:, cols(i)], dst_ref=rx2.at[:, cols(i)],
            send_sem=s2.at[i], recv_sem=r2.at[i], device_id=(t, peer), device_id_type=MESH)

    def fourth(i):
        return pltpu.make_async_remote_copy(
            src_ref=lin.at[:, cols(i)], dst_ref=lrx.at[:, cols(i)],
            send_sem=s4.at[i], recv_sem=r4.at[i], device_id=(t, mate), device_id_type=MESH)

    local = lax.broadcasted_iota(jnp.int32, (own, 1), 0)

    def pick(i, values, block):
        rows = []
        base = local + block * own
        for j in range(ids.shape[0]):
            hit = ids[j:j + 1, cols(i)] == base
            rows.append(jnp.sum(jnp.where(hit, values, F32(0)), axis=0, keepdims=True))
        return jnp.concatenate(rows, axis=0)

    def stage_a(i):
        x_in[i].wait()
        if i + 2 * ahead < n:
            x_in[i + 2 * ahead].start()
        r = lax.dot_general(wt[...], xv[cols(i)], (((1,), (1,)), ((), ())), preferred_element_type=F32)
        part[:, :, :, cols(i)] = r.reshape(2, 2, own, widths[i])
        first(i).start()

    grain = float(int(30000 / (2 * xv.shape[1] * TOKEN_BOUND * GATE_BOUND)))

    def step_of(whole):
        return whole * F32(1.0 / (grain * TOP_CODE))

    def stage_b(i):
        first(i).wait_recv()
        give = part[1 - y, c, :, cols(i)] + rx1[1 - y, :, cols(i)]
        held = part[y, c, :, cols(i)] + rx1[y, :, cols(i)]
        keep[:, cols(i)] = held
        largest = jnp.max(jnp.maximum(jnp.abs(give), jnp.abs(held)), axis=0, keepdims=True)
        whole = jnp.floor(largest * grain) + 1.0
        inverse = F32(grain * TOP_CODE) / whole
        code = jnp.round(give * inverse)
        chosen = jnp.round(pick(i, held, e) * inverse)
        tail = jnp.concatenate([chosen, jnp.broadcast_to(whole, chosen.shape)], axis=0)
        tx2[0:own, cols(i)] = code.astype(jnp.int32).astype(LINK)
        tx2[own:, cols(i)] = tail.astype(jnp.int32).astype(LINK)
        second(i).start()
        lin[:, cols(i)] = pick(i, code, peer) * step_of(whole)
        mine[:, cols(i)] = chosen * step_of(whole)

    def stage_c(i):
        second(i).wait_recv()
        code = rx2[0:own, cols(i)].astype(jnp.int32).astype(F32)
        tail = rx2[own:, cols(i)].astype(jnp.int32).astype(F32)
        top = ids.shape[0]
        step = step_of(tail[top:top + 1])
        logits = keep[:, cols(i)] + code * step
        ours = mine[:, cols(i)] + pick(i, code, e) * step
        theirs = lin[:, cols(i)] + tail[0:top] * step
        lin[:, cols(i)] = ours + theirs
        fourth(i).start()
        affv[:, cols(i)] = 1.0 / (1.0 + jnp.exp(-logits))

    def stage_d(i):
        fourth(i).wait_recv()
        chosen = 1.0 / (1.0 + jnp.exp(-(lin[:, cols(i)] + lrx[:, cols(i)])))
        wtsv[:, cols(i)] = 2.5 * chosen / jnp.sum(chosen, axis=0, keepdims=True)

    def merge_counts():
        for copy in share_out:
            copy.wait()
        cnt[0] = (cnt_a[0] + cnt_a[1]) + (cnt_a[2] + cnt_a[3])
        for copy in cnt_out:
            copy.start()

    def finish_counts():
        for copy in cnt_out + bias_out:
            copy.wait()
        total = cnt[0]
        for d in range(1, ntok):
            total = total + cnt[d]
        load = total[0:1].astype(F32)
        load_ref[...] = load
        target = F32(ntok * ids.shape[1] * ids.shape[0])
        gap = target - F32(experts) * load
        sign = jnp.where(gap > 0, F32(1), jnp.where(gap < 0, F32(-1), F32(0)))
        b0, b1, b2, b3 = (bias_all[k, 0:1] for k in range(4))
        near = jnp.where(c == 0, b0, b1), jnp.where(c == 0, b1, b0)
        far = jnp.where(c == 0, b2, b3), jnp.where(c == 0, b3, b2)
        low = [jnp.where(y == 0, p, q) for p, q in zip(near, far)]
        high = [jnp.where(y == 0, q, p) for p, q in zip(near, far)]
        bias = jnp.concatenate(low + high, axis=1)
        newb_ref[...] = bias + 0.001 * sign

    lag_b, lag_c, lag_d = 2, 7, 8
    for step in range(n + lag_d):
        if step < n:
            stage_a(step)
        if 0 <= step - lag_b < n:
            stage_b(step - lag_b)
        if step == n // 2:
            merge_counts()
        if step == n + lag_b:
            finish_counts()
        if 0 <= step - lag_c < n:
            stage_c(step - lag_c)
        if 0 <= step - lag_d < n:
            stage_d(step - lag_d)
    for i in range(n):
        first(i).wait_send()
        second(i).wait_send()
        fourth(i).wait_send()


def place(aff, wts, load, newb, aff_hbm, wts_hbm, load_hbm, newb_hbm, sem):
    copies = [pltpu.make_async_copy(a, b, sem.at[k]) for k, (a, b) in enumerate(
        ((aff, aff_hbm), (wts, wts_hbm), (load, load_hbm), (newb, newb_hbm)))]
    for copy in copies:
        copy.start()
    for copy in copies:
        copy.wait()


def local(ntok, tokens, gate_weight, expert_ids, expert_bias):
    rows, depth = tokens.shape
    experts = gate_weight.shape[1]
    own = expert_bias.shape[0]
    top = expert_ids.shape[1]
    piece = 256
    widths = [piece // 2] * 2 + [piece] * (rows // piece - 2) + [piece // 2] * 2
    n = len(widths)
    dma = pltpu.SemaphoreType.DMA
    vm = pltpu.VMEM
    any_ = pl.BlockSpec(memory_space=pl.ANY)
    vmem = pl.BlockSpec(memory_space=pltpu.VMEM)
    shapes = ((own, rows), (top, rows), (1, experts), (1, experts))
    results = pl.pallas_call(
        functools.partial(kernel, ntok, widths),
        out_shape=tuple(pltpu.VMEM(shape, F32) for shape in shapes),
        in_specs=[any_] * 4,
        out_specs=(vmem,) * 4,
        scratch_shapes=[
            vm((rows, depth), tokens.dtype), vm((depth, experts), gate_weight.dtype),
            vm((experts, depth), gate_weight.dtype), vm((top, rows), jnp.int32),
            vm((1, own), F32), vm((4, 8, own), F32),
            vm((2, 2, own, rows), F32), vm((2, own, rows), F32), vm((own, rows), F32),
            vm((own + 2 * top, rows), LINK), vm((own + 2 * top, rows), LINK),
            vm((top, rows), F32), vm((top, rows), F32), vm((top, rows), F32),
            vm((4, 8, experts), jnp.int32), vm((ntok, 8, experts), jnp.int32),
            dma((n,)), dma, dma, dma, dma((n,)), dma((n,)), dma((n,)), dma((n,)),
            dma((n,)), dma((n,)), dma((4,)), dma((4,)), dma((ntok,)), dma((ntok,)), dma((4,)), dma((4,)),
        ],
        compiler_params=pltpu.CompilerParams(
            collective_id=0, has_side_effects=True, vmem_limit_bytes=60 * 1024 * 1024),
    )(tokens, gate_weight, expert_ids.T, expert_bias.reshape(1, own))
    aff, wts, load, newb = pl.pallas_call(
        place,
        out_shape=tuple(jax.ShapeDtypeStruct(shape, F32) for shape in shapes),
        in_specs=[vmem] * 4,
        out_specs=(pl.BlockSpec(memory_space=pltpu.HBM),) * 4,
        scratch_shapes=[dma((4,))],
    )(*(pltpu.with_memory_space_constraint(r, pltpu.VMEM) for r in results))
    return aff.T, wts.T, load.reshape(experts), newb.reshape(experts)


def solution(mesh):
    in_specs = (P("tok", "exp"), P("exp", None), P("tok", None), P("exp"))
    out_specs = (P("tok", "exp"), P("tok", None), P(), P())
    return jax.shard_map(functools.partial(local, mesh.shape["tok"]), mesh=mesh,
                         in_specs=in_specs, out_specs=out_specs, check_vma=False)
```

```python
import functools

import jax
import jax.numpy as jnp
from jax import lax
from jax.experimental import pallas as pl
from jax.experimental.pallas import tpu as pltpu
from jax.sharding import PartitionSpec as P

MESH = pl.DeviceIdType.MESH
F32 = jnp.float32
LINK = jnp.int16
TOP_CODE = 32760.0
TOKEN_BOUND, GATE_BOUND = 6.0, 0.0625


def kernel(ntok, widths, x_hbm, w_hbm, ids_hbm, bias_hbm,
           affv, wtsv, load_ref, newb_ref,
           xv, wv, wt, ids, bias_own, bias_all, part, rx1, keep, tx2, rx2, mine, lin, lrx,
           cnt_a, cnt,
           x_sem, w_sem, i_sem, b_sem, s1, r1, s2, r2, s4, r4, sa, ra, sc, rc, sb, rb):
    own = bias_own.shape[1]
    n = len(widths)
    starts = [sum(widths[:i]) for i in range(n)]
    t, e = lax.axis_index("tok"), lax.axis_index("exp")
    y, c = e // 2, e % 2
    mate = 2 * y + 1 - c
    peer = 2 * (1 - y) + c
    cross = 2 * (1 - y) + 1 - c
    experts = 4 * own

    def cols(i):
        return pl.ds(starts[i], widths[i])

    ids_in = pltpu.make_async_copy(ids_hbm, ids, i_sem)
    b_in = pltpu.make_async_copy(bias_hbm, bias_own, b_sem)
    w_in = pltpu.make_async_copy(w_hbm, wv, w_sem)
    x_in = [pltpu.make_async_copy(x_hbm.at[cols(i)], xv.at[cols(i)], x_sem.at[i]) for i in range(n)]
    w_in.start()
    ids_in.start()
    b_in.start()
    ahead = 2
    for copy in x_in[:ahead]:
        copy.start()

    barrier = pltpu.get_barrier_semaphore()
    for other in (mate, peer, cross):
        pl.semaphore_signal(barrier, inc=1, device_id=(t, other), device_id_type=MESH)
    bits = [1 << k for k in range(ntok.bit_length() - 1)]
    pairs = [t + bit - 2 * bit * ((t // bit) % 2) for bit in bits]
    for other in pairs:
        pl.semaphore_signal(barrier, inc=1, device_id=(other, e), device_id_type=MESH)

    ids_in.wait()
    lanes = 128
    share = ids.shape[1] // 4
    numbers = lax.broadcasted_iota(jnp.int32, (experts, lanes), 0).astype(F32).astype(jnp.bfloat16)
    one, zero = jnp.bfloat16(1), jnp.bfloat16(0)
    acc = jnp.zeros((experts, lanes), jnp.bfloat16)
    for g in range(share // lanes):
        at = pl.multiple_of(e * share + g * lanes, lanes)
        found = ids[:, pl.ds(at, lanes)].astype(F32).astype(jnp.bfloat16)
        for j in range(ids.shape[0]):
            acc = acc + jnp.where(found[j:j + 1] == numbers, one, zero)
    counts = lax.dot_general(jnp.ones((8, lanes), jnp.bfloat16), acc,
                             (((1,), (1,)), ((), ())), preferred_element_type=F32)
    cnt_a[0] = counts.astype(jnp.int32)
    b_in.wait()
    bias_all[0] = jnp.broadcast_to(bias_own[...], bias_all.shape[1:])
    w_in.wait()
    for copy in x_in[ahead:2 * ahead]:
        copy.start()
    wt[...] = wv[...].T

    pl.semaphore_wait(barrier, 3 + len(pairs))

    group = ((1, mate), (2, peer), (3, cross))
    share_out = [pltpu.make_async_remote_copy(
        src_ref=cnt_a.at[0], dst_ref=cnt_a.at[k], send_sem=sa.at[k], recv_sem=ra.at[k],
        device_id=(t, other), device_id_type=MESH) for k, other in group]
    bias_out = [pltpu.make_async_remote_copy(
        src_ref=bias_own, dst_ref=bias_all.at[k, pl.ds(0, 1)], send_sem=sb.at[k], recv_sem=rb.at[k],
        device_id=(t, other), device_id_type=MESH) for k, other in group]
    cnt_out = [pltpu.make_async_remote_copy(
        src_ref=cnt.at[2 * k], dst_ref=cnt.at[2 * k + 1], send_sem=sc.at[k], recv_sem=rc.at[k],
        device_id=(other, e), device_id_type=MESH) for k, other in enumerate(pairs)]
    for copy in share_out + bias_out:
        copy.start()

    def first(i):
        return pltpu.make_async_remote_copy(
            src_ref=part.at[:, 1 - c, :, cols(i)], dst_ref=rx1.at[:, :, cols(i)],
            send_sem=s1.at[i], recv_sem=r1.at[i], device_id=(t, mate), device_id_type=MESH)

    def second(i):
        return pltpu.make_async_remote_copy(
            src_ref=tx2.at[:, cols(i)], dst_ref=rx2.at[:, cols(i)],
            send_sem=s2.at[i], recv_sem=r2.at[i], device_id=(t, peer), device_id_type=MESH)

    def fourth(i):
        return pltpu.make_async_remote_copy(
            src_ref=lin.at[:, cols(i)], dst_ref=lrx.at[:, cols(i)],
            send_sem=s4.at[i], recv_sem=r4.at[i], device_id=(t, mate), device_id_type=MESH)

    local = lax.broadcasted_iota(jnp.int32, (own, 1), 0)

    def pick(i, values, block):
        rows = []
        base = local + block * own
        for j in range(ids.shape[0]):
            hit = ids[j:j + 1, cols(i)] == base
            rows.append(jnp.sum(jnp.where(hit, values, F32(0)), axis=0, keepdims=True))
        return jnp.concatenate(rows, axis=0)

    def stage_a(i):
        x_in[i].wait()
        if i + 2 * ahead < n:
            x_in[i + 2 * ahead].start()
        r = lax.dot_general(wt[...], xv[cols(i)], (((1,), (1,)), ((), ())), preferred_element_type=F32)
        part[:, :, :, cols(i)] = r.reshape(2, 2, own, widths[i])
        first(i).start()

    grain = float(int(30000 / (2 * xv.shape[1] * TOKEN_BOUND * GATE_BOUND)))

    def step_of(whole):
        return whole * F32(1.0 / (grain * TOP_CODE))

    def stage_b(i):
        first(i).wait_recv()
        give = part[1 - y, c, :, cols(i)] + rx1[1 - y, :, cols(i)]
        held = part[y, c, :, cols(i)] + rx1[y, :, cols(i)]
        keep[:, cols(i)] = held
        largest = jnp.max(jnp.maximum(jnp.abs(give), jnp.abs(held)), axis=0, keepdims=True)
        whole = jnp.floor(largest * grain) + 1.0
        inverse = F32(grain * TOP_CODE) / whole
        code = jnp.round(give * inverse)
        chosen = jnp.round(pick(i, held, e) * inverse)
        tail = jnp.concatenate([chosen, jnp.broadcast_to(whole, chosen.shape)], axis=0)
        tx2[0:own, cols(i)] = code.astype(jnp.int32).astype(LINK)
        tx2[own:, cols(i)] = tail.astype(jnp.int32).astype(LINK)
        second(i).start()
        lin[:, cols(i)] = pick(i, code, peer) * step_of(whole)
        mine[:, cols(i)] = chosen * step_of(whole)

    def stage_c(i):
        second(i).wait_recv()
        code = rx2[0:own, cols(i)].astype(jnp.int32).astype(F32)
        tail = rx2[own:, cols(i)].astype(jnp.int32).astype(F32)
        top = ids.shape[0]
        step = step_of(tail[top:top + 1])
        logits = keep[:, cols(i)] + code * step
        ours = mine[:, cols(i)] + pick(i, code, e) * step
        theirs = lin[:, cols(i)] + tail[0:top] * step
        lin[:, cols(i)] = ours + theirs
        fourth(i).start()
        affv[:, cols(i)] = 1.0 / (1.0 + jnp.exp(-logits))

    def stage_d(i):
        fourth(i).wait_recv()
        chosen = 1.0 / (1.0 + jnp.exp(-(lin[:, cols(i)] + lrx[:, cols(i)])))
        wtsv[:, cols(i)] = 2.5 * chosen / jnp.sum(chosen, axis=0, keepdims=True)

    def merge_counts():
        for copy in share_out:
            copy.wait()
        cnt[0] = (cnt_a[0] + cnt_a[1]) + (cnt_a[2] + cnt_a[3])
        cnt_out[0].start()

    def double_counts(k):
        cnt_out[k].wait()
        cnt[2 * k + 2] = cnt[2 * k] + cnt[2 * k + 1]
        if k + 1 < len(pairs):
            cnt_out[k + 1].start()

    def finish_counts():
        for copy in bias_out:
            copy.wait()
        total = cnt[2 * len(pairs)]
        load = total[0:1].astype(F32)
        load_ref[...] = load
        target = F32(ntok * ids.shape[1] * ids.shape[0])
        gap = target - F32(experts) * load
        sign = jnp.where(gap > 0, F32(1), jnp.where(gap < 0, F32(-1), F32(0)))
        b0, b1, b2, b3 = (bias_all[k, 0:1] for k in range(4))
        near = jnp.where(c == 0, b0, b1), jnp.where(c == 0, b1, b0)
        far = jnp.where(c == 0, b2, b3), jnp.where(c == 0, b3, b2)
        low = [jnp.where(y == 0, p, q) for p, q in zip(near, far)]
        high = [jnp.where(y == 0, q, p) for p, q in zip(near, far)]
        bias = jnp.concatenate(low + high, axis=1)
        newb_ref[...] = bias + 0.001 * sign

    lag_b, lag_c, lag_d = 2, 7, 8
    spacing = (n + lag_d - 2 - n // 2) // len(pairs)
    for step in range(n + lag_d):
        if step < n:
            stage_a(step)
        if 0 <= step - lag_b < n:
            stage_b(step - lag_b)
        if step == n // 2:
            merge_counts()
        for k in range(len(pairs)):
            if step == n // 2 + (k + 1) * spacing:
                double_counts(k)
                if k + 1 == len(pairs):
                    finish_counts()
        if 0 <= step - lag_c < n:
            stage_c(step - lag_c)
        if 0 <= step - lag_d < n:
            stage_d(step - lag_d)
    for i in range(n):
        first(i).wait_send()
        second(i).wait_send()
        fourth(i).wait_send()


def place(aff, wts, load, newb, aff_hbm, wts_hbm, load_hbm, newb_hbm, sem):
    copies = [pltpu.make_async_copy(a, b, sem.at[k]) for k, (a, b) in enumerate(
        ((aff, aff_hbm), (wts, wts_hbm), (load, load_hbm), (newb, newb_hbm)))]
    for copy in copies:
        copy.start()
    for copy in copies:
        copy.wait()


def local(ntok, tokens, gate_weight, expert_ids, expert_bias):
    rows, depth = tokens.shape
    experts = gate_weight.shape[1]
    own = expert_bias.shape[0]
    top = expert_ids.shape[1]
    piece = 256
    widths = [piece // 2] * 2 + [piece] * (rows // piece - 1)
    n = len(widths)
    dma = pltpu.SemaphoreType.DMA
    vm = pltpu.VMEM
    any_ = pl.BlockSpec(memory_space=pl.ANY)
    vmem = pl.BlockSpec(memory_space=pltpu.VMEM)
    shapes = ((own, rows), (top, rows), (1, experts), (1, experts))
    results = pl.pallas_call(
        functools.partial(kernel, ntok, widths),
        out_shape=tuple(pltpu.VMEM(shape, F32) for shape in shapes),
        in_specs=[any_] * 4,
        out_specs=(vmem,) * 4,
        scratch_shapes=[
            vm((rows, depth), tokens.dtype), vm((depth, experts), gate_weight.dtype),
            vm((experts, depth), gate_weight.dtype), vm((top, rows), jnp.int32),
            vm((1, own), F32), vm((4, 8, own), F32),
            vm((2, 2, own, rows), F32), vm((2, own, rows), F32), vm((own, rows), F32),
            vm((own + 2 * top, rows), LINK), vm((own + 2 * top, rows), LINK),
            vm((top, rows), F32), vm((top, rows), F32), vm((top, rows), F32),
            vm((4, 8, experts), jnp.int32), vm((ntok, 8, experts), jnp.int32),
            dma((n,)), dma, dma, dma, dma((n,)), dma((n,)), dma((n,)), dma((n,)),
            dma((n,)), dma((n,)), dma((4,)), dma((4,)), dma((ntok,)), dma((ntok,)), dma((4,)), dma((4,)),
        ],
        compiler_params=pltpu.CompilerParams(
            collective_id=0, has_side_effects=True, vmem_limit_bytes=60 * 1024 * 1024),
    )(tokens, gate_weight, expert_ids.T, expert_bias.reshape(1, own))
    aff, wts, load, newb = pl.pallas_call(
        place,
        out_shape=tuple(jax.ShapeDtypeStruct(shape, F32) for shape in shapes),
        in_specs=[vmem] * 4,
        out_specs=(pl.BlockSpec(memory_space=pltpu.HBM),) * 4,
        scratch_shapes=[dma((4,))],
    )(*(pltpu.with_memory_space_constraint(r, pltpu.VMEM) for r in results))
    return aff.T, wts.T, load.reshape(experts), newb.reshape(experts)


def solution(mesh):
    in_specs = (P("tok", "exp"), P("exp", None), P("tok", None), P("exp"))
    out_specs = (P("tok", "exp"), P("tok", None), P(), P())
    return jax.shard_map(functools.partial(local, mesh.shape["tok"]), mesh=mesh,
                         in_specs=in_specs, out_specs=out_specs, check_vma=False)
```
